32 devices in a mesh: gx: 4 (over z), gy: 4 (over y, x), gz: 2 (over core).
Axes of the slice: x: 2, y: 2, z: 4, core: 2. Of those that a mesh axis runs over, the one named last changes fastest.
Arguments:
- velocity: float32 [3, 32, 64, 256], P(None, 'gx', 'gy', 'gz'), may hold values from -6 to 6
- density: float32 [32, 64, 256], P('gx', 'gy', 'gz'), may hold values from 0 to 2
- offsets: int32 [3, 32, 64, 256], P(None, 'gx', 'gy', 'gz'), may hold values from -4 to 3
- eighths: int32 [3, 32, 64, 256], P(None, 'gx', 'gy', 'gz'), may hold values from 0 to 7
Outputs:
- new_velocity: float32 [3, 32, 64, 256], P(None, 'gx', 'gy', 'gz')
- new_density: float32 [32, 64, 256], P('gx', 'gy', 'gz')
- pressure: float32 [32, 64, 256], P('gx', 'gy', 'gz')
The draws below stay inside these ranges and needn't reach their ends.
All inputs are finite; a program needn't handle non-finite values.
Results may differ from the reference program's by a relative error of at most 0.00002.
Values sent between devices are 32-bit elements; how exact they have to be, the bound alone decides.
A program may use at most 64 MiB of HBM per device.

```python
import jax
import jax.numpy as jnp
from jax import lax

NX = 32
NY = 64
NZ = 256


def set_ends(values, key, low, high):
    index_at = [jax.random.randint(jax.random.fold_in(key, axis), (), 0, length) for axis, length in enumerate(values.shape)]
    main_axis = values.shape.index(max(values.shape))
    next_to = index_at[:main_axis] + [(index_at[main_axis] + 1) % values.shape[main_axis]] + index_at[main_axis + 1:]
    return values.at[tuple(index_at)].set(low).at[tuple(next_to)].set(high)


def block_levels(key, dims, split, smallest, top_value):
    def one(dim, blocks):
        steps = jax.random.uniform(jax.random.fold_in(jax.random.fold_in(key, 6), dim), (blocks,), jnp.float32, smallest / len(split), top_value / len(split))
        return jnp.repeat(jnp.exp(steps), dims[dim] // blocks).reshape((-1,) + (1,) * (len(dims) - dim - 1))

    level = one(*split[0])
    for cut in split[1:]:
        level = level * one(*cut)
    return level


def noise(own_key, shape, width, limit, shards=(), held_as=jnp.bfloat16):
    gain = block_levels(own_key, shape, shards, -0.22, 0.18) if shards else 1.0
    array = jax.random.normal(own_key, shape, jnp.float32) * width * gain
    return jnp.minimum(jnp.maximum(array, -limit), limit).astype(held_as)


def setup_inputs(seed: int = 0) -> dict:
    key_list = jax.random.split(jax.random.key(seed), 5)
    velocity = noise(key_list[0], (3, NX, NY, NZ), 1.0, 6.0, ((1, 4), (2, 4), (3, 2)), jnp.float32)
    density = jnp.clip(2.0 * jax.random.uniform(key_list[1], (NX, NY, NZ), jnp.float32) ** block_levels(key_list[1], (NX, NY, NZ), ((0, 4), (1, 4), (2, 2)), -0.2, 0.2), 0.0, 2.0)
    offsets = set_ends(jax.random.randint(key_list[2], (3, NX, NY, NZ), -4, 4), jax.random.fold_in(key_list[2], 1), -4, 3).astype(jnp.int32)
    eighths = set_ends(jax.random.randint(key_list[3], (3, NX, NY, NZ), 0, 8), jax.random.fold_in(key_list[3], 1), 0, 7).astype(jnp.int32)
    return dict(velocity=velocity, density=density, offsets=offsets, eighths=eighths)


RELAX_WEIGHT = 6.0 / 7.0


def neighbours(padded):
    summed = padded[2:, 1:-1, 1:-1] + padded[:-2, 1:-1, 1:-1]
    summed = summed + padded[1:-1, 2:, 1:-1] + padded[1:-1, :-2, 1:-1]
    summed = summed + padded[1:-1, 1:-1, 2:] + padded[1:-1, 1:-1, :-2]
    return summed


def operate(padded):
    return 6.0 * padded[1:-1, 1:-1, 1:-1] - neighbours(padded)


def advect_block(padded, offsets, eighths):
    field_count = padded.shape[0]
    stride_y = padded.shape[3]
    stride_x = padded.shape[2] * padded.shape[3]
    flattened = padded.reshape(field_count, -1)
    box_shape = offsets.shape[1:]
    base_x = lax.broadcasted_iota(jnp.int32, box_shape, 0) + 4 + offsets[0]
    base_y = lax.broadcasted_iota(jnp.int32, box_shape, 1) + 4 + offsets[1]
    base_z = lax.broadcasted_iota(jnp.int32, box_shape, 2) + 4 + offsets[2]
    fraction = eighths.astype(jnp.float32) / 8.0
    summed = jnp.zeros((field_count,) + box_shape, jnp.float32)
    for shift_x in (0, 1):
        weight_x = fraction[0] if shift_x else 1.0 - fraction[0]
        for shift_y in (0, 1):
            weight_y = fraction[1] if shift_y else 1.0 - fraction[1]
            for shift_z in (0, 1):
                weight_z = fraction[2] if shift_z else 1.0 - fraction[2]
                weight = weight_x * weight_y * weight_z
                position = (base_x + shift_x) * stride_x + (base_y + shift_y) * stride_y + base_z + shift_z
                picked = jnp.take(flattened, position.reshape(-1), axis=1).reshape(summed.shape)
                summed = summed + weight[None] * picked
    return summed


def divergence_of(velocity_pad):
    part_x = velocity_pad[0, 2:, 1:-1, 1:-1] - velocity_pad[0, :-2, 1:-1, 1:-1]
    part_y = velocity_pad[1, 1:-1, 2:, 1:-1] - velocity_pad[1, 1:-1, :-2, 1:-1]
    part_z = velocity_pad[2, 1:-1, 1:-1, 2:] - velocity_pad[2, 1:-1, 1:-1, :-2]
    return 0.5 * (part_x + part_y + part_z)


def gradient_of(pressure_pad):
    part_x = pressure_pad[2:, 1:-1, 1:-1] - pressure_pad[:-2, 1:-1, 1:-1]
    part_y = pressure_pad[1:-1, 2:, 1:-1] - pressure_pad[1:-1, :-2, 1:-1]
    part_z = pressure_pad[1:-1, 1:-1, 2:] - pressure_pad[1:-1, 1:-1, :-2]
    return 0.5 * jnp.stack([part_x, part_y, part_z], axis=0)


def restrict(field):
    return field.reshape(field.shape[0] // 2, 2, field.shape[1] // 2, 2, field.shape[2] // 2, 2).mean(axis=(1, 3, 5))


def prolong(field):
    return jnp.repeat(jnp.repeat(jnp.repeat(field, 2, axis=0), 2, axis=1), 2, axis=2)


def sweeps(source, spacing):
    relaxation = RELAX_WEIGHT / 6.0
    first_sweep = relaxation * spacing * source
    second_sweep = first_sweep + relaxation * (spacing * source - operate(jnp.pad(first_sweep, 1)))
    return second_sweep


def smooth_level(source, spacing):
    second_sweep = sweeps(source, spacing)
    residual = source - operate(jnp.pad(second_sweep, 1)) / spacing
    return second_sweep, residual


def reference(velocity, density, offsets, eighths):
    fields = jnp.concatenate([velocity, density[None]], axis=0)
    padded = jnp.pad(fields, ((0, 0), (4, 4), (4, 4), (4, 4)))
    advected = advect_block(padded, offsets, eighths)
    velocity_pad = jnp.pad(advected[:3], ((0, 0), (1, 1), (1, 1), (1, 1)))
    divergence = divergence_of(velocity_pad)
    fine_sweep, fine_residual = smooth_level(-divergence, 1.0)
    middle_sweep, middle_residual = smooth_level(restrict(fine_residual), 4.0)
    coarse_sweep = sweeps(restrict(middle_residual), 16.0)
    pressure = fine_sweep + prolong(middle_sweep + prolong(coarse_sweep))
    gradient = gradient_of(jnp.pad(pressure, 1))
    return advected[:3] - gradient, advected[3], pressure
```

```python
import functools

import jax
import jax.numpy as jnp
from jax import lax
from jax.experimental import pallas as pl
from jax.experimental.pallas import tpu as pltpu
from jax.sharding import PartitionSpec as P

MESH = pl.DeviceIdType.MESH
RELAX = (6.0 / 7.0) / 6.0
HALO = 4
XY = [(dx, dy) for dx in (-1, 0, 1) for dy in (-1, 0, 1) if (dx, dy) != (0, 0)]
FAR = [(dx, dy) for dx in (-2, -1, 0, 1, 2) for dy in (-1, 0, 1) if (dx, dy) != (0, 0)]


def lanes(shape):
    return lax.broadcasted_iota(jnp.int32, shape, len(shape) - 1)


def roll(x, shift, axis):
    shift = shift % x.shape[axis]
    return x if shift == 0 else pltpu.roll(x, shift, axis)


def inside(sizes, me, delta):
    ok = None
    for n, i, d in zip(sizes, me, delta):
        if d:
            one = (i + d >= 0) & (i + d < n)
            ok = one if ok is None else ok & one
    return ok


class Comm:
    def __init__(self, sizes, me, send, recv):
        self.sizes, self.me, self.send, self.recv = sizes, me, send, recv
        self.copies = []

    def add(self, delta, src, dst, slot):
        device = tuple(i + d for i, d in zip(self.me, delta))
        copy = pltpu.make_async_remote_copy(
            src_ref=src, dst_ref=dst, send_sem=self.send.at[slot], recv_sem=self.recv.at[slot],
            device_id=device, device_id_type=MESH,
        )
        to = inside(self.sizes, self.me, delta)
        source = inside(self.sizes, self.me, tuple(-d for d in delta))
        pl.when(to)(copy.start)
        self.copies.append((copy, to, source))

    def wait(self):
        for copy, to, source in self.copies:
            pl.when(source)(copy.wait_recv)
        for copy, to, source in self.copies:
            pl.when(to)(copy.wait_send)


def zero_if_missing(sizes, me, delta, ref):
    @pl.when(jnp.logical_not(inside(sizes, me, delta)))
    def _():
        ref[...] = jnp.zeros(ref.shape, ref.dtype)


def pick_x(d):
    return {-1: 0, 1: 1}[d]


def exchange_xy(sizes, me, own, strips, rx, ry, rc, sems, out, zero=True):
    f, p, r, _ = own.shape
    for i in range(p):
        strips[0, :, i] = own[:, i, 0:HALO, :]
        strips[1, :, i] = own[:, i, r - HALO : r, :]
    comm = Comm(sizes, me, *sems)
    for slot, (dx, dy) in enumerate(XY):
        xs = slice(0, HALO) if dx < 0 else slice(p - HALO, p)
        if dy == 0:
            src, dst = own.at[:, xs], rx.at[pick_x(-dx)]
        elif dx == 0:
            src, dst = strips.at[pick_x(dy)], ry.at[pick_x(-dy)]
        else:
            src, dst = strips.at[pick_x(dy), :, xs], rc.at[pick_x(-dx), pick_x(-dy)]
        comm.add((dx, dy, 0), src, dst, slot)
    for dx, dy in XY:
        ref = rx.at[pick_x(dx)] if dy == 0 else ry.at[pick_x(dy)] if dx == 0 else rc.at[pick_x(dx), pick_x(dy)]
        zero_if_missing(sizes, me, (dx, dy, 0), ref)
    out[:, HALO : HALO + p, HALO : HALO + r, :] = own[...]
    comm.wait()
    for sx, xs in ((0, slice(0, HALO)), (1, slice(HALO + p, HALO + p + HALO))):
        out[:, xs, HALO : HALO + r, :] = rx[sx]
        for sy, ys in ((0, slice(0, HALO)), (1, slice(HALO + r, HALO + r + HALO))):
            out[:, xs, ys, :] = rc[sx, sy]
    for sy, ys in ((0, slice(0, HALO)), (1, slice(HALO + r, HALO + r + HALO))):
        out[:, HALO : HALO + p, ys, :] = ry[sy]


def exchange_z(sizes, me, own, got, sems):
    comm = Comm(sizes, me, *sems)
    comm.add((0, 0, -1), own, got.at[1], 0)
    comm.add((0, 0, 1), own, got.at[0], 1)
    zero_if_missing(sizes, me, (0, 0, -1), got.at[0])
    zero_if_missing(sizes, me, (0, 0, 1), got.at[1])
    comm.wait()


def pack_z(ext, packed):
    f, p, rows, _ = ext.shape
    lane = lanes((rows, 128))
    for c in range(f):
        total = roll(ext[c, 0], 4, 1)
        for x in range(1, p):
            total = jnp.where(lane >= 8 * x, roll(ext[c, x], 4 + 8 * x, 1), total)
        packed[c] = total


def gather(x, index):
    return jnp.take_along_axis(x, index, axis=1, mode="promise_in_bounds")


def advect_tile(code, load, shift):
    ox, oy, oz = code & 7, (code >> 3) & 7, (code >> 6) & 7
    fx = ((code >> 9) & 7).astype(jnp.float32) * 0.125
    fy = ((code >> 12) & 7).astype(jnp.float32) * 0.125
    fz = ((code >> 15) & 7).astype(jnp.float32) * 0.125
    low = (lanes((8, 128)) + oz + shift) & 127
    high = (low + 1) & 127

    def weight(o, frac, step):
        return jnp.where(o == step, 1.0 - frac, jnp.where(o == step - 1, frac, 0.0))

    wy = [weight(oy, fy, dy) for dy in range(9)]
    totals = [None] * 4
    for dx in range(9):
        wx = weight(ox, fx, dx)
        wx0, wx1 = wx * (1.0 - fz), wx * fz
        for c in range(4):
            a0 = a1 = None
            for dy in range(9):
                rows = load(c, dx, dy)
                g0, g1 = wy[dy] * gather(rows, low), wy[dy] * gather(rows, high)
                a0 = g0 if a0 is None else a0 + g0
                a1 = g1 if a1 is None else a1 + g1
            value = wx0 * a0 + wx1 * a1
            totals[c] = value if totals[c] is None else totals[c] + value
    return totals


def kernel(sizes, vel, den, off, eig, new_vel, new_den, press, fields, stripA, rxA, ryA, rcA, ext, packed,
           gotP, srcA, srcB, code, codeB, resB, u, stripB, rxB, ryB, rcB, extU, packU, gotU, wide, s0, q0, r0,
           tmp0, own1, strip1, rx1, ry1, rc1, ext1, got1, wide1, q1, r1, tmp1, own2, got2, ext2, gotz2, sum1, fine,
           sxyA, rxyA, szA, rzA, sxyB, rxyB, szB, rzB, sxy1, rxy1, sz1, rz1, sxy2, rxy2, sz2, rz2):
    me = tuple(lax.axis_index(a) for a in ("gx", "gy", "gz"))
    p, r = den.shape[0], den.shape[1]
    fields[0:3] = vel[...]
    fields[3] = den[...]

    barrier = pltpu.get_barrier_semaphore()
    peers = [(dx, dy, 0) for dx, dy in FAR] + [(0, 0, -1), (0, 0, 1)]
    count = jnp.int32(0)
    for delta in peers:
        ok = inside(sizes, me, delta)

        @pl.when(ok)
        def _():
            pl.semaphore_signal(barrier, inc=1, device_id=tuple(i + d for i, d in zip(me, delta)), device_id_type=MESH)

        count = count + jnp.where(ok, 1, 0)
    pl.semaphore_wait(barrier, count)

    whole = (off[0] + 4) + 8 * (off[1] + 4) + 64 * (off[2] + 4)
    code[...] = whole + 512 * eig[0] + 4096 * eig[1] + 32768 * eig[2]
    lane16 = lanes((r, 128))
    total = roll(code[0], 12, 1)
    for g in range(1, p):
        total = jnp.where(lane16 >= 16 * g, roll(code[g], 16 * g + 12, 1), total)
    codeB[...] = total

    exchange_xy(sizes, me, fields, stripA, rxA, ryA, rcA, (sxyA, rxyA), ext)
    pack_z(ext, packed)
    exchange_z(sizes, me, packed, gotP, (szA, rzA))

    rows = r + 8
    lane = lanes((rows, 128))
    for c in range(4):
        below, above = gotP[0, c], gotP[1, c]
        halves = []
        for h in range(2):
            total = None
            for g in range(8):
                x = 8 * h + g
                main = ext[c, x]
                srcA[c, x] = jnp.where(lane < 4, roll(below, -8 * x, 1), roll(main, 4, 1))
                piece = jnp.where((lane & 15) < 12, roll(main, 16 * g + 12, 1), roll(above, 8 * g + 8 - 64 * h, 1))
                total = piece if total is None else jnp.where(lane >= 16 * g, piece, total)
            halves.append(total)
        for dx in range(9):
            if dx == 8:
                srcB[c, dx] = halves[1]
            else:
                srcB[c, dx] = jnp.where(lane < 128 - 16 * dx, roll(halves[0], -16 * dx, 1), roll(halves[1], -16 * dx, 1))

    for half in range(r // 8):
        y0 = 8 * half
        totals = advect_tile(codeB[y0 : y0 + 8], lambda c, dx, dy: srcB[c, dx, y0 + dy : y0 + dy + 8, :], -4)
        for c in range(4):
            resB[c, y0 : y0 + 8] = totals[c]

    def plane(x, carry):
        for half in range(r // 8):
            y0 = 8 * half
            totals = advect_tile(code[x, y0 : y0 + 8], lambda c, dx, dy: srcA[c, x + dx, y0 + dy : y0 + dy + 8, :], 0)
            for c in range(4):
                u[c, x, y0 : y0 + 8] = totals[c]
        return carry

    lax.fori_loop(0, p, plane, 0)
    for c in range(4):
        for x in range(p):
            u[c, x] = jnp.where(lane16 >= 120, roll(resB[c], -(16 * x + 12), 1), u[c, x])
    new_den[...] = u[3]

    vel_u = u.at[0:3]
    exchange_xy(sizes, me, vel_u, stripB, rxB, ryB, rcB, (sxyB, rxyB), extU)
    pack_z(extU, packU)
    exchange_z(sizes, me, packU, gotU, (szB, rzB))
    for c in range(3):
        both = jnp.where((lane & 7) < 4, gotU[0, c], gotU[1, c])
        for x in range(p + 8):
            wide[c, x, :, 0:128] = extU[c, x]
            wide[c, x, :, 128:256] = roll(both, -(8 * x + 4), 1)

    def yz_mask(nrows, first_row, block_rows, cells):
        row = lax.broadcasted_iota(jnp.int32, (nrows, 256), 0) - first_row + me[1] * block_rows
        spot = lanes((nrows, 256))
        z = jnp.where(spot < 192, spot, spot - 256) + me[2] * cells
        return (row >= 0) & (row < sizes[1] * block_rows) & (z >= 0) & (z < sizes[2] * cells)

    def x_ok(x, first, block):
        g = x - first + me[0] * block
        return (g >= 0) & (g < sizes[0] * block)

    mask0 = yz_mask(rows, HALO, r, 128)

    def around(ref, x, step):
        v = ref[x]
        total = ref[x + 1] + ref[x - 1]
        total = total + roll(v, -1, 0) + roll(v, 1, 0)
        total = total + roll(v, -step, 1) + roll(v, step, 1)
        return 6.0 * v - total

    def second(ref, x, scale, step):
        v = ref[x]
        first = (RELAX * scale) * v
        return first + RELAX * (scale * v - (RELAX * scale) * around(ref, x, step))

    def source0(x, carry):
        part = wide[0, x + 1] - wide[0, x - 1]
        v = wide[1, x]
        part = part + (roll(v, -1, 0) - roll(v, 1, 0))
        v = wide[2, x]
        part = part + (roll(v, -1, 1) - roll(v, 1, 1))
        s0[x] = jnp.where(mask0 & x_ok(x, HALO, p), -0.5 * part, 0.0)
        return carry

    lax.fori_loop(1, p + 7, source0, 0)

    def second0(x, carry):
        q0[x] = jnp.where(mask0 & x_ok(x, HALO, p), second(s0, x, 1.0, 1), 0.0)
        return carry

    lax.fori_loop(2, p + 6, second0, 0)

    def residual0(x, carry):
        r0[x] = (s0[x] - around(q0, x, 1))[:, 0:128]
        return carry

    lax.fori_loop(HALO, HALO + p, residual0, 0)
    lane8 = lanes((r // 2, 128))
    for x in range(p // 2):
        tmp0[...] = r0[HALO + 2 * x] + r0[HALO + 2 * x + 1]
        v = tmp0[pl.ds(HALO, r // 2, stride=2), :] + tmp0[pl.ds(HALO + 1, r // 2, stride=2), :]
        v = v + jnp.where((lane8 & 1) == 0, roll(v, -1, 1), roll(v, 1, 1))
        own1[0, x] = 0.125 * v

    p1, r1n = p // 2, r // 2
    exchange_xy(sizes, me, own1, strip1, rx1, ry1, rc1, (sxy1, rxy1), ext1)
    exchange_z(sizes, me, ext1, got1, (sz1, rz1))
    rows1 = r1n + 8
    lane1 = lanes((rows1, 128))
    for x in range(p1 + 8):
        wide1[x, :, 0:128] = ext1[0, x]
        wide1[x, :, 128:256] = jnp.where(lane1 < 64, got1[1, 0, x], got1[0, 0, x])
    mask1 = yz_mask(rows1, HALO, r1n, 128)
    for x in range(HALO - 1, HALO + p1 + 1):
        q1[x] = jnp.where(mask1 & x_ok(x, HALO, p1), second(wide1, x, 4.0, 2), 0.0)
    for x in range(HALO, HALO + p1):
        r1[x] = (wide1[x] - 0.25 * around(q1, x, 2))[:, 0:128]
    p2, r2n = p1 // 2, r1n // 2
    lane4 = lanes((r2n, 128))
    for x in range(p2):
        tmp1[...] = r1[HALO + 2 * x] + r1[HALO + 2 * x + 1]
        v = tmp1[pl.ds(HALO, r2n, stride=2), :] + tmp1[pl.ds(HALO + 1, r2n, stride=2), :]
        v = v + jnp.where((lane4 & 3) < 2, roll(v, -2, 1), roll(v, 2, 1))
        own2[x] = 0.125 * v

    comm = Comm(sizes, me, sxy2, rxy2)
    for slot, (dx, dy) in enumerate(FAR):
        comm.add((dx, dy, 0), own2, got2.at[2 - dx, 1 - dy], slot)
    for dx, dy in FAR:
        zero_if_missing(sizes, me, (dx, dy, 0), got2.at[dx + 2, dy + 1])
    got2[2, 1] = own2[...]
    ext2[...] = jnp.zeros(ext2.shape, jnp.float32)
    comm.wait()
    for a in range(5):
        for b in range(3):
            ext2[p2 * a : p2 * a + p2, r2n * b : r2n * b + r2n, :] = got2[a, b]
    exchange_z(sizes, me, ext2, gotz2, (sz2, rz2))
    lane2 = lanes((16, 128))
    mask2 = yz_mask(16, r2n, r2n, 128)
    planes2 = {}
    for x in range(2 * p2 - 2, 3 * p2 + 2):
        planes2[x] = jnp.concatenate([ext2[x], jnp.where(lane2 < 64, gotz2[1, x], gotz2[0, x])], axis=1)
    sum1[...] = jnp.zeros(sum1.shape, jnp.float32)
    for x in range(2 * p2 - 1, 3 * p2 + 1):
        v = jnp.where(mask2 & x_ok(x, 2 * p2, p2), second(planes2, x, 16.0, 4), 0.0)
        first_row = r2n - 1
        take = r2n + 2
        base = HALO - 2
        for side in range(2):
            part = v[first_row : first_row + take, 128 * side : 128 * side + 128]
            sum1[x, side, pl.ds(base, take, stride=2), :] = part
            sum1[x, side, pl.ds(base + 1, take, stride=2), :] = part
    for x1 in range(HALO - 1, HALO + p1 + 1):
        x2 = (x1 - HALO) // 2 + 2 * p2
        for side in range(2):
            v = q1[x1, :, 128 * side : 128 * side + 128] + sum1[x2, side]
            part = v[HALO - 2 : HALO - 2 + r1n + 4]
            fine[x1, side, pl.ds(0, r1n + 4, stride=2), :] = part
            fine[x1, side, pl.ds(1, r1n + 4, stride=2), :] = part
    for x in range(HALO - 1, HALO + p + 1):
        x1 = (x - HALO) // 2 + HALO
        coarse = jnp.concatenate([fine[x1, 0], fine[x1, 1]], axis=1)
        s0[x] = jnp.where(mask0 & x_ok(x, HALO, p), q0[x] + coarse, 0.0)
    for x in range(p):
        v = s0[x + HALO]
        cut = lambda t: t[HALO : HALO + r, 0:128]
        press[x] = cut(v)
        new_vel[0, x] = u[0, x] - 0.5 * cut(s0[x + HALO + 1] - s0[x + HALO - 1])
        new_vel[1, x] = u[1, x] - 0.5 * cut(roll(v, -1, 0) - roll(v, 1, 0))
        new_vel[2, x] = u[2, x] - 0.5 * cut(roll(v, -1, 1) - roll(v, 1, 1))


def step(sizes, velocity, density, offsets, eighths):
    p, r, _ = density.shape
    f32 = jnp.float32

    def vm(*shape):
        return pltpu.VMEM(shape, f32)

    def xy(f, p, r):
        return [vm(2, f, p, 4, 128), vm(2, f, 4, r, 128), vm(2, f, p, 4, 128), vm(2, 2, f, 4, 4, 128)]

    p1, r1, p2, r2 = p // 2, r // 2, p // 4, r // 4
    rows, rows1 = r + 8, r1 + 8
    dma = lambda n: pltpu.SemaphoreType.DMA((n,))
    scratch = (
        [vm(4, p, r, 128)] + xy(4, p, r)
        + [vm(4, p + 8, rows, 128), vm(4, rows, 128), vm(2, 4, rows, 128), vm(4, p + 8, rows, 128),
           vm(4, 9, rows, 128), pltpu.VMEM((p, r, 128), jnp.int32), pltpu.VMEM((r, 128), jnp.int32),
           vm(4, r, 128), vm(4, p, r, 128)]
        + xy(3, p, r)
        + [vm(3, p + 8, rows, 128), vm(3, rows, 128), vm(2, 3, rows, 128), vm(3, p + 8, rows, 256),
           vm(p + 8, rows, 256), vm(p + 8, rows, 256), vm(p + 8, rows, 128), vm(rows, 128), vm(1, p1, r1, 128)]
        + xy(1, p1, r1)
        + [vm(1, p1 + 8, rows1, 128), vm(2, 1, p1 + 8, rows1, 128), vm(p1 + 8, rows1, 256), vm(p1 + 8, rows1, 256),
           vm(p1 + 8, rows1, 128), vm(rows1, 128), vm(p2, r2, 128), vm(5, 3, p2, r2, 128), vm(5 * p2, 16, 128),
           vm(2, 5 * p2, 16, 128), vm(5 * p2, 2, rows1, 128), vm(p1 + 8, 2, rows, 128)]
        + [dma(8), dma(8), dma(2), dma(2)] * 3 + [dma(14), dma(14), dma(2), dma(2)]
    )
    vmem = pl.BlockSpec(memory_space=pltpu.VMEM)
    return pl.pallas_call(
        functools.partial(kernel, sizes),
        out_shape=(
            jax.ShapeDtypeStruct(velocity.shape, f32),
            jax.ShapeDtypeStruct(density.shape, f32),
            jax.ShapeDtypeStruct(density.shape, f32),
        ),
        in_specs=[vmem] * 4,
        out_specs=(vmem,) * 3,
        scratch_shapes=scratch,
        compiler_params=pltpu.CompilerParams(
            collective_id=0, has_side_effects=True, vmem_limit_bytes=48 * 1024 * 1024
        ),
    )(velocity, density, offsets, eighths)


def solution(mesh):
    sizes = tuple(mesh.shape[a] for a in ("gx", "gy", "gz"))
    block = P("gx", "gy", "gz")
    stacked = P(None, "gx", "gy", "gz")
    return jax.shard_map(
        functools.partial(step, sizes),
        mesh=mesh,
        in_specs=(stacked, block, stacked, stacked),
        out_specs=(stacked, block, block),
        check_vma=False,
    )
```

```python
import functools

import jax
import jax.numpy as jnp
from jax import lax
from jax.experimental import pallas as pl
from jax.experimental.pallas import tpu as pltpu
from jax.sharding import PartitionSpec as P

MESH = pl.DeviceIdType.MESH
RELAX = (6.0 / 7.0) / 6.0
HALO = 4
XY = [(dx, dy) for dx in (-1, 0, 1) for dy in (-1, 0, 1) if (dx, dy) != (0, 0)]
FAR = [(dx, dy) for dx in (-2, -1, 0, 1, 2) for dy in (-1, 0, 1) if (dx, dy) != (0, 0)]


def lanes(shape):
    return lax.broadcasted_iota(jnp.int32, shape, len(shape) - 1)


def roll(x, shift, axis):
    shift = shift % x.shape[axis]
    return x if shift == 0 else pltpu.roll(x, shift, axis)


def inside(sizes, me, delta):
    ok = None
    for n, i, d in zip(sizes, me, delta):
        if d:
            one = (i + d >= 0) & (i + d < n)
            ok = one if ok is None else ok & one
    return ok


class Comm:
    def __init__(self, sizes, me, send, recv):
        self.sizes, self.me, self.send, self.recv = sizes, me, send, recv
        self.copies = []

    def add(self, delta, src, dst, slot):
        device = tuple(i + d for i, d in zip(self.me, delta))
        copy = pltpu.make_async_remote_copy(
            src_ref=src, dst_ref=dst, send_sem=self.send.at[slot], recv_sem=self.recv.at[slot],
            device_id=device, device_id_type=MESH,
        )
        to = inside(self.sizes, self.me, delta)
        source = inside(self.sizes, self.me, tuple(-d for d in delta))
        pl.when(to)(copy.start)
        self.copies.append((copy, to, source))

    def wait(self):
        for copy, to, source in self.copies:
            pl.when(source)(copy.wait_recv)
        for copy, to, source in self.copies:
            pl.when(to)(copy.wait_send)


def zero_if_missing(sizes, me, delta, ref):
    @pl.when(jnp.logical_not(inside(sizes, me, delta)))
    def _():
        ref[...] = jnp.zeros(ref.shape, ref.dtype)


def pick_x(d):
    return {-1: 0, 1: 1}[d]


def exchange_xy(sizes, me, own, strips, rx, ry, rc, sems, out, meanwhile=None):
    f, p, r, _ = own.shape
    for i in range(p):
        strips[0, :, i] = own[:, i, 0:HALO, :]
        strips[1, :, i] = own[:, i, r - HALO : r, :]
    comm = Comm(sizes, me, *sems)
    for slot, (dx, dy) in enumerate(XY):
        xs = slice(0, HALO) if dx < 0 else slice(p - HALO, p)
        if dy == 0:
            src, dst = own.at[:, xs], rx.at[pick_x(-dx)]
        elif dx == 0:
            src, dst = strips.at[pick_x(dy)], ry.at[pick_x(-dy)]
        else:
            src, dst = strips.at[pick_x(dy), :, xs], rc.at[pick_x(-dx), pick_x(-dy)]
        comm.add((dx, dy, 0), src, dst, slot)
    for dx, dy in XY:
        ref = rx.at[pick_x(dx)] if dy == 0 else ry.at[pick_x(dy)] if dx == 0 else rc.at[pick_x(dx), pick_x(dy)]
        zero_if_missing(sizes, me, (dx, dy, 0), ref)
    out[:, HALO : HALO + p, HALO : HALO + r, :] = own[...]
    if meanwhile is not None:
        meanwhile()
    comm.wait()
    for sx, xs in ((0, slice(0, HALO)), (1, slice(HALO + p, HALO + p + HALO))):
        out[:, xs, HALO : HALO + r, :] = rx[sx]
        for sy, ys in ((0, slice(0, HALO)), (1, slice(HALO + r, HALO + r + HALO))):
            out[:, xs, ys, :] = rc[sx, sy]
    for sy, ys in ((0, slice(0, HALO)), (1, slice(HALO + r, HALO + r + HALO))):
        out[:, HALO : HALO + p, ys, :] = ry[sy]


def exchange_z(sizes, me, own, got, sems):
    comm = Comm(sizes, me, *sems)
    comm.add((0, 0, -1), own, got.at[1], 0)
    comm.add((0, 0, 1), own, got.at[0], 1)
    zero_if_missing(sizes, me, (0, 0, -1), got.at[0])
    zero_if_missing(sizes, me, (0, 0, 1), got.at[1])
    comm.wait()


def pack_z(ext, packed):
    f, p, rows, _ = ext.shape
    lane = lanes((rows, 128))
    for c in range(f):
        total = roll(ext[c, 0], 4, 1)
        for x in range(1, p):
            total = jnp.where(lane >= 8 * x, roll(ext[c, x], 4 + 8 * x, 1), total)
        packed[c] = total


def gather(x, index):
    return jnp.take_along_axis(x, index, axis=1, mode="promise_in_bounds")


def advect_tile(code, load, shift):
    ox, oy, oz = code & 7, (code >> 3) & 7, (code >> 6) & 7
    fx = ((code >> 9) & 7).astype(jnp.float32) * 0.125
    fy = ((code >> 12) & 7).astype(jnp.float32) * 0.125
    fz = ((code >> 15) & 7).astype(jnp.float32) * 0.125
    low = (lanes((8, 128)) + oz + shift) & 127
    high = (low + 1) & 127

    def weight(o, frac, step):
        return jnp.where(o == step, 1.0 - frac, jnp.where(o == step - 1, frac, 0.0))

    wy = [weight(oy, fy, dy) for dy in range(9)]
    totals = [None] * 4
    for dx in range(9):
        wx = weight(ox, fx, dx)
        wx0, wx1 = wx * (1.0 - fz), wx * fz
        for c in range(4):
            a0 = a1 = None
            for dy in range(9):
                rows = load(c, dx, dy)
                g0, g1 = wy[dy] * gather(rows, low), wy[dy] * gather(rows, high)
                a0 = g0 if a0 is None else a0 + g0
                a1 = g1 if a1 is None else a1 + g1
            value = wx0 * a0 + wx1 * a1
            totals[c] = value if totals[c] is None else totals[c] + value
    return totals


def kernel(sizes, vel, den, off_hbm, eig_hbm, new_vel, new_den, press, off, eig, fetch_sem, fields, stripA, rxA, ryA, rcA, ext, packed,
           gotP, srcA, srcB, code, codeB, resB, u, stripB, rxB, ryB, rcB, extU, packU, gotU, wide, s0, q0, r0,
           tmp0, own1, strip1, rx1, ry1, rc1, ext1, got1, wide1, q1, r1, tmp1, own2, got2, ext2, gotz2, sum1, fine,
           sxyA, rxyA, szA, rzA, sxyB, rxyB, szB, rzB, sxy1, rxy1, sz1, rz1, sxy2, rxy2, sz2, rz2):
    me = tuple(lax.axis_index(a) for a in ("gx", "gy", "gz"))
    p, r = den.shape[0], den.shape[1]
    fetch = [pltpu.make_async_copy(off_hbm, off, fetch_sem.at[0]), pltpu.make_async_copy(eig_hbm, eig, fetch_sem.at[1])]
    for copy in fetch:
        copy.start()
    fields[0:3] = vel[...]
    fields[3] = den[...]

    barrier = pltpu.get_barrier_semaphore()
    peers = [(dx, dy, 0) for dx, dy in FAR] + [(0, 0, -1), (0, 0, 1)]
    count = jnp.int32(0)
    for delta in peers:
        ok = inside(sizes, me, delta)

        @pl.when(ok)
        def _():
            pl.semaphore_signal(barrier, inc=1, device_id=tuple(i + d for i, d in zip(me, delta)), device_id_type=MESH)

        count = count + jnp.where(ok, 1, 0)
    pl.semaphore_wait(barrier, count)

    def positions():
        for copy in fetch:
            copy.wait()
        whole = (off[0] + 4) + 8 * (off[1] + 4) + 64 * (off[2] + 4)
        code[...] = whole + 512 * eig[0] + 4096 * eig[1] + 32768 * eig[2]
        lane16 = lanes((r, 128))
        total = roll(code[0], 12, 1)
        for g in range(1, p):
            total = jnp.where(lane16 >= 16 * g, roll(code[g], 16 * g + 12, 1), total)
        codeB[...] = total

    exchange_xy(sizes, me, fields, stripA, rxA, ryA, rcA, (sxyA, rxyA), ext, positions)
    pack_z(ext, packed)
    exchange_z(sizes, me, packed, gotP, (szA, rzA))

    rows = r + 8
    lane16 = lanes((r, 128))
    lane = lanes((rows, 128))
    for c in range(4):
        below, above = gotP[0, c], gotP[1, c]
        halves = []
        for h in range(2):
            total = None
            for g in range(8):
                x = 8 * h + g
                main = ext[c, x]
                srcA[c, x] = jnp.where(lane < 4, roll(below, -8 * x, 1), roll(main, 4, 1))
                piece = jnp.where((lane & 15) < 12, roll(main, 16 * g + 12, 1), roll(above, 8 * g + 8 - 64 * h, 1))
                total = piece if total is None else jnp.where(lane >= 16 * g, piece, total)
            halves.append(total)
        for dx in range(9):
            if dx == 8:
                srcB[c, dx] = halves[1]
            else:
                srcB[c, dx] = jnp.where(lane < 128 - 16 * dx, roll(halves[0], -16 * dx, 1), roll(halves[1], -16 * dx, 1))

    for half in range(r // 8):
        y0 = 8 * half
        totals = advect_tile(codeB[y0 : y0 + 8], lambda c, dx, dy: srcB[c, dx, y0 + dy : y0 + dy + 8, :], -4)
        for c in range(4):
            resB[c, y0 : y0 + 8] = totals[c]

    for half in range(r // 8):
        y0 = 8 * half

        def plane(x, carry, y0=y0):
            totals = advect_tile(code[x, y0 : y0 + 8], lambda c, dx, dy: srcA[c, x + dx, y0 + dy : y0 + dy + 8, :], 0)
            for c in range(4):
                u[c, x, y0 : y0 + 8] = totals[c]
            return carry

        lax.fori_loop(0, p, plane, 0)
    for c in range(4):
        for x in range(p):
            u[c, x] = jnp.where(lane16 >= 120, roll(resB[c], -(16 * x + 12), 1), u[c, x])
    new_den[...] = u[3]

    vel_u = u.at[0:3]
    exchange_xy(sizes, me, vel_u, stripB, rxB, ryB, rcB, (sxyB, rxyB), extU)
    pack_z(extU, packU)
    exchange_z(sizes, me, packU, gotU, (szB, rzB))
    for c in range(3):
        both = jnp.where((lane & 7) < 4, gotU[0, c], gotU[1, c])
        for x in range(p + 8):
            wide[c, x, :, 0:128] = extU[c, x]
            wide[c, x, :, 128:256] = roll(both, -(8 * x + 4), 1)

    def yz_mask(nrows, first_row, block_rows, cells):
        row = lax.broadcasted_iota(jnp.int32, (nrows, 256), 0) - first_row + me[1] * block_rows
        spot = lanes((nrows, 256))
        z = jnp.where(spot < 192, spot, spot - 256) + me[2] * cells
        return (row >= 0) & (row < sizes[1] * block_rows) & (z >= 0) & (z < sizes[2] * cells)

    def x_ok(x, first, block):
        g = x - first + me[0] * block
        return (g >= 0) & (g < sizes[0] * block)

    mask0 = yz_mask(rows, HALO, r, 128)

    def around(ref, x, step):
        v = ref[x]
        total = ref[x + 1] + ref[x - 1]
        total = total + roll(v, -1, 0) + roll(v, 1, 0)
        total = total + roll(v, -step, 1) + roll(v, step, 1)
        return 6.0 * v - total

    def second(ref, x, scale, step):
        v = ref[x]
        first = (RELAX * scale) * v
        return first + RELAX * (scale * v - (RELAX * scale) * around(ref, x, step))

    def source0(x, carry):
        part = wide[0, x + 1] - wide[0, x - 1]
        v = wide[1, x]
        part = part + (roll(v, -1, 0) - roll(v, 1, 0))
        v = wide[2, x]
        part = part + (roll(v, -1, 1) - roll(v, 1, 1))
        s0[x] = jnp.where(mask0 & x_ok(x, HALO, p), -0.5 * part, 0.0)
        return carry

    lax.fori_loop(1, p + 7, source0, 0)

    def second0(x, carry):
        q0[x] = jnp.where(mask0 & x_ok(x, HALO, p), second(s0, x, 1.0, 1), 0.0)
        return carry

    lax.fori_loop(2, p + 6, second0, 0)

    def residual0(x, carry):
        r0[x] = (s0[x] - around(q0, x, 1))[:, 0:128]
        return carry

    lax.fori_loop(HALO, HALO + p, residual0, 0)
    lane8 = lanes((r // 2, 128))
    for x in range(p // 2):
        tmp0[...] = r0[HALO + 2 * x] + r0[HALO + 2 * x + 1]
        v = tmp0[pl.ds(HALO, r // 2, stride=2), :] + tmp0[pl.ds(HALO + 1, r // 2, stride=2), :]
        v = v + jnp.where((lane8 & 1) == 0, roll(v, -1, 1), roll(v, 1, 1))
        own1[0, x] = 0.125 * v

    p1, r1n = p // 2, r // 2
    exchange_xy(sizes, me, own1, strip1, rx1, ry1, rc1, (sxy1, rxy1), ext1)
    exchange_z(sizes, me, ext1, got1, (sz1, rz1))
    rows1 = r1n + 8
    lane1 = lanes((rows1, 128))
    for x in range(p1 + 8):
        wide1[x, :, 0:128] = ext1[0, x]
        wide1[x, :, 128:256] = jnp.where(lane1 < 64, got1[1, 0, x], got1[0, 0, x])
    mask1 = yz_mask(rows1, HALO, r1n, 128)
    for x in range(HALO - 1, HALO + p1 + 1):
        q1[x] = jnp.where(mask1 & x_ok(x, HALO, p1), second(wide1, x, 4.0, 2), 0.0)
    for x in range(HALO, HALO + p1):
        r1[x] = (wide1[x] - 0.25 * around(q1, x, 2))[:, 0:128]
    p2, r2n = p1 // 2, r1n // 2
    lane4 = lanes((r2n, 128))
    for x in range(p2):
        tmp1[...] = r1[HALO + 2 * x] + r1[HALO + 2 * x + 1]
        v = tmp1[pl.ds(HALO, r2n, stride=2), :] + tmp1[pl.ds(HALO + 1, r2n, stride=2), :]
        v = v + jnp.where((lane4 & 3) < 2, roll(v, -2, 1), roll(v, 2, 1))
        own2[x] = 0.125 * v

    comm = Comm(sizes, me, sxy2, rxy2)
    for slot, (dx, dy) in enumerate(FAR):
        comm.add((dx, dy, 0), own2, got2.at[2 - dx, 1 - dy], slot)
    for dx, dy in FAR:
        zero_if_missing(sizes, me, (dx, dy, 0), got2.at[dx + 2, dy + 1])
    got2[2, 1] = own2[...]
    ext2[...] = jnp.zeros(ext2.shape, jnp.float32)
    comm.wait()
    for a in range(5):
        for b in range(3):
            ext2[p2 * a : p2 * a + p2, r2n * b : r2n * b + r2n, :] = got2[a, b]
    exchange_z(sizes, me, ext2, gotz2, (sz2, rz2))
    lane2 = lanes((16, 128))
    mask2 = yz_mask(16, r2n, r2n, 128)
    planes2 = {}
    for x in range(2 * p2 - 2, 3 * p2 + 2):
        planes2[x] = jnp.concatenate([ext2[x], jnp.where(lane2 < 64, gotz2[1, x], gotz2[0, x])], axis=1)
    sum1[...] = jnp.zeros(sum1.shape, jnp.float32)
    for x in range(2 * p2 - 1, 3 * p2 + 1):
        v = jnp.where(mask2 & x_ok(x, 2 * p2, p2), second(planes2, x, 16.0, 4), 0.0)
        first_row = r2n - 1
        take = r2n + 2
        base = HALO - 2
        for side in range(2):
            part = v[first_row : first_row + take, 128 * side : 128 * side + 128]
            sum1[x, side, pl.ds(base, take, stride=2), :] = part
            sum1[x, side, pl.ds(base + 1, take, stride=2), :] = part
    for x1 in range(HALO - 1, HALO + p1 + 1):
        x2 = (x1 - HALO) // 2 + 2 * p2
        for side in range(2):
            v = q1[x1, :, 128 * side : 128 * side + 128] + sum1[x2, side]
            part = v[HALO - 2 : HALO - 2 + r1n + 4]
            fine[x1, side, pl.ds(0, r1n + 4, stride=2), :] = part
            fine[x1, side, pl.ds(1, r1n + 4, stride=2), :] = part
    for x in range(HALO - 1, HALO + p + 1):
        x1 = (x - HALO) // 2 + HALO
        coarse = jnp.concatenate([fine[x1, 0], fine[x1, 1]], axis=1)
        s0[x] = jnp.where(mask0 & x_ok(x, HALO, p), q0[x] + coarse, 0.0)
    for x in range(p):
        v = s0[x + HALO]
        cut = lambda t: t[HALO : HALO + r, 0:128]
        press[x] = cut(v)
        new_vel[0, x] = u[0, x] - 0.5 * cut(s0[x + HALO + 1] - s0[x + HALO - 1])
        new_vel[1, x] = u[1, x] - 0.5 * cut(roll(v, -1, 0) - roll(v, 1, 0))
        new_vel[2, x] = u[2, x] - 0.5 * cut(roll(v, -1, 1) - roll(v, 1, 1))


def step(sizes, velocity, density, offsets, eighths):
    p, r, _ = density.shape
    f32 = jnp.float32

    def vm(*shape):
        return pltpu.VMEM(shape, f32)

    def xy(f, p, r):
        return [vm(2, f, p, 4, 128), vm(2, f, 4, r, 128), vm(2, f, p, 4, 128), vm(2, 2, f, 4, 4, 128)]

    p1, r1, p2, r2 = p // 2, r // 2, p // 4, r // 4
    rows, rows1 = r + 8, r1 + 8
    dma = lambda n: pltpu.SemaphoreType.DMA((n,))
    scratch = (
        [pltpu.VMEM(offsets.shape, jnp.int32), pltpu.VMEM(eighths.shape, jnp.int32), dma(2), vm(4, p, r, 128)] + xy(4, p, r)
        + [vm(4, p + 8, rows, 128), vm(4, rows, 128), vm(2, 4, rows, 128), vm(4, p + 8, rows, 128),
           vm(4, 9, rows, 128), pltpu.VMEM((p, r, 128), jnp.int32), pltpu.VMEM((r, 128), jnp.int32),
           vm(4, r, 128), vm(4, p, r, 128)]
        + xy(3, p, r)
        + [vm(3, p + 8, rows, 128), vm(3, rows, 128), vm(2, 3, rows, 128), vm(3, p + 8, rows, 256),
           vm(p + 8, rows, 256), vm(p + 8, rows, 256), vm(p + 8, rows, 128), vm(rows, 128), vm(1, p1, r1, 128)]
        + xy(1, p1, r1)
        + [vm(1, p1 + 8, rows1, 128), vm(2, 1, p1 + 8, rows1, 128), vm(p1 + 8, rows1, 256), vm(p1 + 8, rows1, 256),
           vm(p1 + 8, rows1, 128), vm(rows1, 128), vm(p2, r2, 128), vm(5, 3, p2, r2, 128), vm(5 * p2, 16, 128),
           vm(2, 5 * p2, 16, 128), vm(5 * p2, 2, rows1, 128), vm(p1 + 8, 2, rows, 128)]
        + [dma(8), dma(8), dma(2), dma(2)] * 3 + [dma(14), dma(14), dma(2), dma(2)]
    )
    vmem = pl.BlockSpec(memory_space=pltpu.VMEM)
    return pl.pallas_call(
        functools.partial(kernel, sizes),
        out_shape=(
            jax.ShapeDtypeStruct(velocity.shape, f32),
            jax.ShapeDtypeStruct(density.shape, f32),
            jax.ShapeDtypeStruct(density.shape, f32),
        ),
        in_specs=[vmem] * 2 + [pl.BlockSpec(memory_space=pltpu.HBM)] * 2,
        out_specs=(vmem,) * 3,
        scratch_shapes=scratch,
        compiler_params=pltpu.CompilerParams(
            collective_id=0, has_side_effects=True, vmem_limit_bytes=48 * 1024 * 1024
        ),
    )(velocity, density, offsets, eighths)


def solution(mesh):
    sizes = tuple(mesh.shape[a] for a in ("gx", "gy", "gz"))
    block = P("gx", "gy", "gz")
    stacked = P(None, "gx", "gy", "gz")
    return jax.shard_map(
        functools.partial(step, sizes),
        mesh=mesh,
        in_specs=(stacked, block, stacked, stacked),
        out_specs=(stacked, block, block),
        check_vma=False,
    )
```
